32 devices in a mesh: rep: 1, fsdp: 32 (over z, y, x, core).
Axes of the slice: x: 2, y: 2, z: 4, core: 2. Of those that a mesh axis runs over, the one named last changes fastest.
Arguments:
- accumulated: bfloat16 [1, 2048, 14336], P('rep', 'fsdp'), may hold values from -6 to 6
- q_start: bfloat16 [32, 14336], P(None, 'fsdp'), may hold values from -6 to 6
Outputs:
- residual_buffer: bfloat16 [1, 2048, 14336], P('rep', 'fsdp')
- basis_f32: float32 [2048, 32], P('fsdp')
- q_factor: float32 [32, 14336], P(None, 'fsdp')
The draws below stay inside these ranges and needn't reach their ends.
All inputs are finite; a program needn't handle non-finite values.
Results may differ from the reference program's by a relative error of at most 0.0039.
Values may be sent and summed in bfloat16 or wider, within the bound.
No kernel may reach another device: no remote copies, remote signals or barrier semaphores. Data moves between devices by JAX's collectives and lax.ppermute only.
A program may use at most 64 MiB of HBM per device.

```python
import jax
import jax.numpy as jnp
from jax import lax

COLS = 14336
RANK = 32
ITERS = 2
ROWS = 2048
N_REP = 1


def raised(drawn, own_key, source, target, shards_of, factor):
    def block_of(dim):
        return (jnp.arange(drawn.shape[dim]) // (drawn.shape[dim] // shards_of)).reshape((-1,) + (1,) * (drawn.ndim - 1 - dim))

    one_side = jax.random.permutation(own_key, shards_of)[block_of(target)]
    second = (block_of(target) + shards_of // 2) % shards_of
    return jnp.where((block_of(source) == one_side) | (block_of(source) == second), factor * drawn, drawn)


def level_of(key, extent, split, low, largest):
    level = 1.0
    for position, shards_of in split:
        heights = jax.random.uniform(jax.random.fold_in(jax.random.fold_in(key, 6), position), (shards_of,), jnp.float32, low / len(split), largest / len(split))
        level = level * jnp.repeat(jnp.exp(heights), extent[position] // shards_of).reshape((-1,) + (1,) * (len(extent) - 1 - position))
    return level


def scatter_about(own_key, shape, deviation, reach, cuts=(), dtype=jnp.bfloat16):
    values = jax.random.normal(own_key, shape, jnp.float32) * deviation
    if len(cuts) > 0:
        values = level_of(own_key, shape, cuts, -0.22, 0.18) * values
    return jnp.clip(values, min=-reach, max=reach).astype(dtype)


def gaussian_with(rng, shape, scale, bound, cuts, heavy, held_as=jnp.bfloat16):
    result = scale * jax.random.normal(rng, shape, jnp.float32)
    if cuts:
        result = result * level_of(rng, shape, cuts, -0.22, 0.18)
    return jnp.clip(raised(result, jax.random.fold_in(rng, 3), *heavy), -bound, bound).astype(held_as)


def setup_inputs(seed: int = 0) -> dict:
    seeds = jax.random.split(jax.random.key(seed), 3)
    return {
        "accumulated": gaussian_with(seeds[0], (N_REP, ROWS, COLS), 1.0, 6.0, ((1, 32),), (1, 2, 32, 2.75)),
        "q_start": scatter_about(seeds[1], (RANK, COLS), 1.0, 6.0, ((1, 32),)),
    }


def orthonormal(p_sum):
    gram_matrix = jnp.dot(p_sum.T, p_sum, precision=lax.Precision.HIGHEST)
    factor = jnp.linalg.cholesky(gram_matrix)
    return lax.linalg.triangular_solve(factor, p_sum, left_side=False, lower=True, transpose_a=True)

def reference(accumulated, q_start):
    right_factor = q_start
    for iteration in range(ITERS):

        def add_product(running, replica_rows):
            term = lax.dot_general(replica_rows.astype(jnp.float32), right_factor.astype(jnp.float32), (((1,), (1,)), ((), ())), preferred_element_type=jnp.float32)
            return (running + term, None)
        p_sum, unused = lax.scan(add_product, jnp.zeros((ROWS, RANK), jnp.float32), accumulated)
        basis_f32 = orthonormal(p_sum)
        basis_bf16 = basis_f32.astype(jnp.bfloat16)

        def add_columns(running, replica_rows):
            term = lax.dot_general(basis_bf16.astype(jnp.float32), replica_rows.astype(jnp.float32), (((0,), (0,)), ((), ())), preferred_element_type=jnp.float32)
            return (running + term, None)
        q_sum, unused = lax.scan(add_columns, jnp.zeros((RANK, COLS), jnp.float32), accumulated)
        q_factor = q_sum / N_REP
        right_factor = q_factor.astype(jnp.bfloat16)
    approx = lax.dot_general(basis_bf16.astype(jnp.float32), right_factor.astype(jnp.float32), (((1,), (0,)), ((), ())), preferred_element_type=jnp.float32)
    residual_buffer = lax.map(lambda replica_rows: (replica_rows.astype(jnp.float32) - approx).astype(jnp.bfloat16), accumulated)
    return (residual_buffer, basis_f32, q_factor)
```

```python
import jax
import jax.numpy as jnp
from jax import lax
from jax.sharding import Mesh, PartitionSpec as P

ITERS = 2
HIGHEST = lax.Precision.HIGHEST
CHIP = ("hi", "lo")
ROWS = ("hi", "lo", "core")
SWAP = ((0, 1), (1, 0))


def transposed_product(left, right):
    return lax.dot_general(left, right, (((0,), (0,)), ((), ())), preferred_element_type=jnp.float32)


def product_transposed(left, right):
    return lax.dot_general(left, right, (((1,), (1,)), ((), ())), preferred_element_type=jnp.float32)


def swap_cores(values):
    return lax.ppermute(values, "core", SWAP)


def spread(values, axis):
    copies = jnp.broadcast_to(values[None], (lax.axis_size(axis),) + values.shape)
    return lax.all_to_all(copies, axis, 0, 0, tiled=True)


def gather_chips(values):
    by_hi = spread(values, "hi")
    return spread(by_hi, "lo").swapaxes(0, 1)


def gather_right(q_half):
    blocks = gather_chips(q_half)
    hi, lo, half, width = blocks.shape
    own = blocks.transpose(2, 0, 1, 3).reshape(half, hi * lo * width)
    return own, swap_cores(own)


def orthonormal_basis(p_rows, p_own):
    own_gram = jnp.dot(p_rows.T, p_rows, precision=HIGHEST)
    gram_matrix = own_gram + swap_cores(own_gram)
    factor = jnp.linalg.cholesky(gram_matrix)
    inverse = lax.linalg.triangular_solve(
        factor, jnp.eye(factor.shape[0], dtype=jnp.float32), left_side=True, lower=True
    )
    basis = lax.dot_general(p_rows, inverse, (((1,), (1,)), ((), ())), precision=HIGHEST)
    basis_own = lax.dot_general(p_own, inverse, (((1,), (1,)), ((), ())), precision=HIGHEST)
    return basis, basis_own


def on_device(accumulated, q_start):
    own_rows = accumulated[0]
    replicas = lax.axis_size("rep")
    chips = lax.axis_size(CHIP)
    core = lax.axis_index("core")
    rows, cols = own_rows.shape
    rank, shard_cols = q_start.shape
    half, width = rank // 2, cols // chips

    blocks = own_rows.reshape(rows, chips, width).transpose(1, 0, 2)
    block = lax.all_to_all(blocks, CHIP, 0, 0, tiled=True).reshape(chips * rows, width)

    kept = lax.dynamic_slice_in_dim(q_start, core * half, half, 0)
    given = lax.dynamic_slice_in_dim(q_start, (1 - core) * half, half, 0)
    taken = swap_cores(given)
    first = jnp.where(core == 0, kept, taken)
    second = jnp.where(core == 0, taken, kept)
    own, other = gather_right(jnp.concatenate([first, second], axis=1))
    p_mine = product_transposed(own_rows, own)
    p_theirs = product_transposed(own_rows, other)
    p_own = jnp.where(
        core == 0,
        jnp.concatenate([p_mine, p_theirs], axis=1),
        jnp.concatenate([p_theirs, p_mine], axis=1),
    )
    for iteration in range(ITERS):
        if iteration > 0:
            term = product_transposed(block, right_factor).reshape(chips, rows, rank)
            p_own = jnp.sum(lax.all_to_all(term, CHIP, 0, 0, tiled=True), axis=0)
        if replicas > 1:
            p_own = lax.psum(p_own, "rep")
        p_rows = spread(p_own, CHIP).reshape(chips * rows, rank)
        basis, basis_own = orthonormal_basis(p_rows, p_own)
        q_term = transposed_product(basis.astype(jnp.bfloat16), block)
        q_chip = q_term + swap_cores(q_term)
        if replicas > 1:
            q_chip = lax.psum(q_chip, "rep")
        q_chip = q_chip / replicas
        right_factor = q_chip.astype(jnp.bfloat16)
    q_owned = lax.dynamic_slice_in_dim(q_chip, core * shard_cols, shard_cols, 1)
    own, other = gather_right(lax.dynamic_slice_in_dim(right_factor, core * half, half, 0))
    basis_bf16 = basis_own.astype(jnp.bfloat16)
    mine = lax.dynamic_slice_in_dim(basis_bf16, core * half, half, 1)
    theirs = lax.dynamic_slice_in_dim(basis_bf16, (1 - core) * half, half, 1)
    approx = lax.dot_general(
        jnp.concatenate([mine, theirs], axis=1),
        jnp.concatenate([own, other], axis=0),
        (((1,), (0,)), ((), ())),
        preferred_element_type=jnp.float32,
    )
    residual_buffer = (own_rows.astype(jnp.float32) - approx).astype(jnp.bfloat16)[None]
    return (residual_buffer, basis_own, q_owned)


def solution(mesh):
    chips = mesh.shape["fsdp"] // 2
    lo = 4
    split = Mesh(
        mesh.devices.reshape(mesh.shape["rep"], chips // lo, lo, 2), ("rep", "hi", "lo", "core")
    )
    in_specs = (P("rep", ROWS, None), P(None, ROWS))
    out_specs = (P("rep", ROWS, None), P(ROWS, None), P(None, ROWS))
    return jax.shard_map(
        on_device, mesh=split, in_specs=in_specs, out_specs=out_specs, check_vma=False
    )
```

```python
import jax
import jax.numpy as jnp
from jax import lax
from jax.sharding import Mesh, PartitionSpec as P


ITERS = 2
HIGHEST = lax.Precision.HIGHEST
CHIP = ("hi", "lo")
ROWS = ("hi", "lo", "core")
SWAP = ((0, 1), (1, 0))


def transposed_product(left, right):
    return lax.dot_general(left, right, (((0,), (0,)), ((), ())), preferred_element_type=jnp.float32)


def product_transposed(left, right):
    return lax.dot_general(left, right, (((1,), (1,)), ((), ())), preferred_element_type=jnp.float32)


def swap_cores(values):
    return lax.ppermute(values, "core", SWAP)


def spread(values, axis):
    copies = jnp.broadcast_to(values[None], (lax.axis_size(axis),) + values.shape)
    return lax.all_to_all(copies, axis, 0, 0, tiled=True)


def doubled(values, axis, dim):
    values = jnp.expand_dims(values, dim)
    position = lax.axis_index(axis)
    size = lax.axis_size(axis)
    bit = 1
    while bit < size:
        pairs = tuple((index, index ^ bit) for index in range(size))
        taken = lax.ppermute(values, axis, pairs)
        upper = (position & bit) != 0
        values = jnp.where(
            upper,
            jnp.concatenate([taken, values], axis=dim),
            jnp.concatenate([values, taken], axis=dim),
        )
        bit *= 2
    return values


def gather_chips(values):
    by_hi = spread(values, "hi")
    return spread(by_hi, "lo").swapaxes(0, 1)


def gather_right(q_half, in_pairs):
    if in_pairs:
        blocks = doubled(doubled(q_half, "hi", 0), "lo", 1)
    else:
        blocks = gather_chips(q_half)
    hi, lo, half, width = blocks.shape
    own = blocks.transpose(2, 0, 1, 3).reshape(half, hi * lo * width)
    return own, swap_cores(own)


def orthonormal_basis(p_rows, p_own):
    own_gram = jnp.dot(p_rows.T, p_rows, precision=HIGHEST)
    gram_matrix = own_gram + swap_cores(own_gram)
    factor = jnp.linalg.cholesky(gram_matrix)
    inverse = lax.linalg.triangular_solve(
        factor, jnp.eye(factor.shape[0], dtype=jnp.float32), left_side=True, lower=True
    )
    basis = lax.dot_general(p_rows, inverse, (((1,), (1,)), ((), ())), precision=HIGHEST)
    basis_own = lax.dot_general(p_own, inverse, (((1,), (1,)), ((), ())), precision=HIGHEST)
    return basis, basis_own


def on_device(accumulated, q_start):
    own_rows = accumulated[0]
    replicas = lax.axis_size("rep")
    chips = lax.axis_size(CHIP)
    core = lax.axis_index("core")
    rows, cols = own_rows.shape
    rank, shard_cols = q_start.shape
    half, width = rank // 2, cols // chips

    blocks = own_rows.reshape(rows, chips, width).transpose(1, 0, 2)
    block = lax.all_to_all(blocks, CHIP, 0, 0, tiled=True).reshape(chips * rows, width)

    kept = lax.dynamic_slice_in_dim(q_start, core * half, half, 0)
    given = lax.dynamic_slice_in_dim(q_start, (1 - core) * half, half, 0)
    taken = swap_cores(given)
    first = jnp.where(core == 0, kept, taken)
    second = jnp.where(core == 0, taken, kept)
    own, other = gather_right(jnp.concatenate([first, second], axis=1), True)
    p_mine = product_transposed(own_rows, own)
    p_theirs = product_transposed(own_rows, other)
    p_own = jnp.where(
        core == 0,
        jnp.concatenate([p_mine, p_theirs], axis=1),
        jnp.concatenate([p_theirs, p_mine], axis=1),
    )
    for iteration in range(ITERS):
        if iteration > 0:
            term = product_transposed(block, right_factor).reshape(chips, rows, rank)
            p_own = jnp.sum(lax.all_to_all(term, CHIP, 0, 0, tiled=True), axis=0)
        if replicas > 1:
            p_own = lax.psum(p_own, "rep")
        if iteration > 0:
            p_rows = spread(p_own, CHIP).reshape(chips * rows, rank)
        else:
            p_rows = doubled(doubled(p_own, "hi", 0), "lo", 1).reshape(chips * rows, rank)
        basis, basis_own = orthonormal_basis(p_rows, p_own)
        q_term = transposed_product(basis.astype(jnp.bfloat16), block)
        q_chip = q_term + swap_cores(q_term)
        if replicas > 1:
            q_chip = lax.psum(q_chip, "rep")
        q_chip = q_chip / replicas
        right_factor = q_chip.astype(jnp.bfloat16)
    q_owned = lax.dynamic_slice_in_dim(q_chip, core * shard_cols, shard_cols, 1)
    own, other = gather_right(lax.dynamic_slice_in_dim(right_factor, core * half, half, 0), False)
    basis_bf16 = basis_own.astype(jnp.bfloat16)
    mine = lax.dynamic_slice_in_dim(basis_bf16, core * half, half, 1)
    theirs = lax.dynamic_slice_in_dim(basis_bf16, (1 - core) * half, half, 1)
    approx = lax.dot_general(
        jnp.concatenate([mine, theirs], axis=1),
        jnp.concatenate([own, other], axis=0),
        (((1,), (0,)), ((), ())),
        preferred_element_type=jnp.float32,
    )
    residual_buffer = (own_rows.astype(jnp.float32) - approx).astype(jnp.bfloat16)[None]
    return (residual_buffer, basis_own, q_owned)


def solution(mesh):
    chips = mesh.shape["fsdp"] // 2
    lo = 4
    split = Mesh(
        mesh.devices.reshape(mesh.shape["rep"], chips // lo, lo, 2), ("rep", "hi", "lo", "core")
    )
    in_specs = (P("rep", ROWS, None), P(None, ROWS))
    out_specs = (P("rep", ROWS, None), P(ROWS, None), P(None, ROWS))
    return jax.shard_map(
        on_device, mesh=split, in_specs=in_specs, out_specs=out_specs, check_vma=False
    )
```

```python
import jax
import jax.numpy as jnp
from jax import lax
from jax.experimental import pallas as pl
from jax.experimental.pallas import tpu as pltpu
from jax.sharding import Mesh, PartitionSpec as P


ITERS = 2
HIGHEST = lax.Precision.HIGHEST
CHIP = ("hi", "lo")
ROWS = ("hi", "lo", "core")
SWAP = ((0, 1), (1, 0))


def transposed_product(left, right):
    return lax.dot_general(left, right, (((0,), (0,)), ((), ())), preferred_element_type=jnp.float32)


def product_transposed(left, right):
    return lax.dot_general(left, right, (((1,), (1,)), ((), ())), preferred_element_type=jnp.float32)


def swap_cores(values):
    return lax.ppermute(values, "core", SWAP)


def spread(values, axis):
    copies = jnp.broadcast_to(values[None], (lax.axis_size(axis),) + values.shape)
    return lax.all_to_all(copies, axis, 0, 0, tiled=True)


def exchanged(values, axis, dim):
    position = lax.axis_index(axis)
    size = lax.axis_size(axis)
    pieces = [values]
    for offset in range(1, size):
        pairs = tuple((index, index ^ offset) for index in range(size))
        pieces.append(lax.ppermute(values, axis, pairs))
    bit = 1
    while bit < size:
        swap = (position & bit) != 0
        pieces = [jnp.where(swap, pieces[i ^ bit], pieces[i]) for i in range(size)]
        bit *= 2
    return jnp.stack(pieces, axis=dim)


def inverse_factor_kernel(own_ref, other_ref, inverse_ref, columns):
    rank = own_ref.shape[0]
    blocks = rank // 8
    gram = own_ref[...] + other_ref[...]
    for j in range(rank):
        column = jnp.broadcast_to(gram[:, j : j + 1], (rank, 128))
        for i in range(j // 8, blocks):
            columns[j, i] = column[8 * i : 8 * i + 8]
    row = lax.broadcasted_iota(jnp.int32, (8, 128), 0)
    lane = lax.broadcasted_iota(jnp.int32, (8, 128), 1)
    solved = [(lane == row + 8 * i).astype(jnp.float32) for i in range(blocks)]
    for k in range(rank):
        top, at = k // 8, k % 8
        pivot = columns[k, top][at : at + 1]
        scale = lax.rsqrt(pivot)
        scale = scale * (1.5 - 0.5 * pivot * scale * scale)
        lower = {i: columns[k, i] * scale for i in range(top, blocks)}
        lower[top] = jnp.where(row > at, lower[top], 0.0)
        solved_row = solved[top][at : at + 1] * scale
        for i in range(top, blocks):
            reduced = solved[i] - lower[i] * solved_row
            solved[i] = jnp.where(row == at, solved_row, reduced) if i == top else reduced
        for j in range(k + 1, rank):
            entry = lower[j // 8][j % 8 : j % 8 + 1]
            for i in range(j // 8, blocks):
                columns[j, i] = columns[j, i] - lower[i] * entry
    for i in range(blocks):
        inverse_ref[8 * i : 8 * i + 8, :] = solved[i][:, :rank]


def inverse_factor(own_gram, other_gram):
    rank = own_gram.shape[0]
    return pl.pallas_call(
        inverse_factor_kernel,
        out_shape=jax.ShapeDtypeStruct((rank, rank), jnp.float32),
        in_specs=[pl.BlockSpec(memory_space=pltpu.VMEM)] * 2,
        out_specs=pl.BlockSpec(memory_space=pltpu.VMEM),
        scratch_shapes=[pltpu.VMEM((rank, rank // 8, 8, 128), jnp.float32)],
        compiler_params=pltpu.CompilerParams(vmem_limit_bytes=4 * 1024 * 1024),
        cost_estimate=pl.CostEstimate(flops=4000000, bytes_accessed=12288, transcendentals=rank),
        name="inverse_factor",
    )(own_gram, other_gram)


def gather_chips(values):
    by_hi = spread(values, "hi")
    return spread(by_hi, "lo").swapaxes(0, 1)


def gather_right(q_half):
    blocks = gather_chips(q_half)
    hi, lo, half, width = blocks.shape
    own = blocks.transpose(2, 0, 1, 3).reshape(half, hi * lo * width)
    return own, swap_cores(own)


def orthonormal_basis(p_rows, p_own):
    own_gram = jnp.dot(p_rows.T, p_rows, precision=HIGHEST)
    inverse = inverse_factor(own_gram, swap_cores(own_gram))
    basis = lax.dot_general(p_rows, inverse, (((1,), (1,)), ((), ())), precision=HIGHEST)
    basis_own = lax.dot_general(p_own, inverse, (((1,), (1,)), ((), ())), precision=HIGHEST)
    return basis, basis_own


def on_device(accumulated, q_start):
    own_rows = accumulated[0]
    replicas = lax.axis_size("rep")
    chips = lax.axis_size(CHIP)
    core = lax.axis_index("core")
    rows, cols = own_rows.shape
    rank, shard_cols = q_start.shape
    half, width = rank // 2, cols // chips

    blocks = own_rows.reshape(rows, chips, width).transpose(1, 0, 2)
    block = lax.all_to_all(blocks, CHIP, 0, 0, tiled=True).reshape(chips * rows, width)

    shift = width - 2 * shard_cols + shard_cols % 128
    placed = jnp.where(
        core == 0, jnp.pad(q_start, ((0, 0), (0, shift))), jnp.pad(q_start, ((0, 0), (shift, 0)))
    )
    by_hi = exchanged(placed, "hi", 0)
    own = exchanged(by_hi, "lo", 1)
    other = swap_cores(own)
    rest = width - shard_cols - shift
    even = jnp.pad(jnp.where(core == 0, own, other), ((0, 0), (0, 0), (0, 0), (0, rest)))
    odd = jnp.pad(jnp.where(core == 0, other, own), ((0, 0), (0, 0), (0, 0), (rest, 0)))
    start = (even + odd).transpose(2, 0, 1, 3).reshape(rank, cols)
    p_own = product_transposed(own_rows, start)
    for iteration in range(ITERS):
        if iteration > 0:
            term = product_transposed(block, right_factor).reshape(chips, rows, rank)
            p_own = jnp.sum(lax.all_to_all(term, CHIP, 0, 0, tiled=True), axis=0)
        if replicas > 1:
            p_own = lax.psum(p_own, "rep")
        if iteration > 0:
            p_rows = spread(p_own, CHIP).reshape(chips * rows, rank)
        else:
            by_lo = exchanged(p_own, "lo", 0)
            p_rows = exchanged(by_lo, "hi", 0).reshape(chips * rows, rank)
        basis, basis_own = orthonormal_basis(p_rows, p_own)
        q_term = transposed_product(basis.astype(jnp.bfloat16), block)
        q_chip = q_term + swap_cores(q_term)
        if replicas > 1:
            q_chip = lax.psum(q_chip, "rep")
        q_chip = q_chip / replicas
        right_factor = q_chip.astype(jnp.bfloat16)
    q_owned = lax.dynamic_slice_in_dim(q_chip, core * shard_cols, shard_cols, 1)
    own, other = gather_right(lax.dynamic_slice_in_dim(right_factor, core * half, half, 0))
    basis_bf16 = basis_own.astype(jnp.bfloat16)
    mine = lax.dynamic_slice_in_dim(basis_bf16, core * half, half, 1)
    theirs = lax.dynamic_slice_in_dim(basis_bf16, (1 - core) * half, half, 1)
    approx = lax.dot_general(
        jnp.concatenate([mine, theirs], axis=1),
        jnp.concatenate([own, other], axis=0),
        (((1,), (0,)), ((), ())),
        preferred_element_type=jnp.float32,
    )
    residual_buffer = (own_rows.astype(jnp.float32) - approx).astype(jnp.bfloat16)[None]
    return (residual_buffer, basis_own, q_owned)


def solution(mesh):
    chips = mesh.shape["fsdp"] // 2
    lo = 4
    split = Mesh(
        mesh.devices.reshape(mesh.shape["rep"], chips // lo, lo, 2), ("rep", "hi", "lo", "core")
    )
    in_specs = (P("rep", ROWS, None), P(None, ROWS))
    out_specs = (P("rep", ROWS, None), P(ROWS, None), P(None, ROWS))
    return jax.shard_map(
        on_device, mesh=split, in_specs=in_specs, out_specs=out_specs, check_vma=False
    )
```

```python
import jax
import jax.numpy as jnp
from jax import lax
from jax.experimental import pallas as pl
from jax.experimental.pallas import tpu as pltpu
from jax.sharding import Mesh, PartitionSpec as P


ITERS = 2
HIGHEST = lax.Precision.HIGHEST
CHIP = ("hi", "lo")
ROWS = ("hi", "lo", "core")
SWAP = ((0, 1), (1, 0))


def swap_cores(values):
    return lax.ppermute(values, "core", SWAP)


def spread(values, axis):
    copies = jnp.broadcast_to(values[None], (lax.axis_size(axis),) + values.shape)
    return lax.all_to_all(copies, axis, 0, 0, tiled=True)


def exchanged(values, axis, dim):
    position = lax.axis_index(axis)
    size = lax.axis_size(axis)
    pieces = [values]
    for offset in range(1, size):
        pairs = tuple((index, index ^ offset) for index in range(size))
        pieces.append(lax.ppermute(values, axis, pairs))
    bit = 1
    while bit < size:
        swap = (position & bit) != 0
        pieces = [jnp.where(swap, pieces[i ^ bit], pieces[i]) for i in range(size)]
        bit *= 2
    return jnp.stack(pieces, axis=dim)


def kernel_call(kernel, out_shape, flops, scratch=()):
    single = not isinstance(out_shape, tuple)
    outs = (out_shape,) if single else out_shape
    vmem = pl.BlockSpec(memory_space=pltpu.VMEM)
    return lambda *args: pl.pallas_call(
        kernel,
        out_shape=out_shape,
        in_specs=[vmem] * len(args),
        out_specs=vmem if single else (vmem,) * len(outs),
        scratch_shapes=list(scratch),
        compiler_params=pltpu.CompilerParams(vmem_limit_bytes=16 * 1024 * 1024),
        cost_estimate=pl.CostEstimate(
            flops=flops, bytes_accessed=sum(a.size * a.dtype.itemsize for a in args), transcendentals=0
        ),
    )(*args)


def packed_rows(wide, groups):
    per = wide.shape[0] // groups
    return jnp.concatenate([wide[per * g : per * g + per, :] for g in range(groups)], axis=1)


def cut_kernel(rows_ref, blocks_ref, held, read_semaphores, write_semaphores):
    chips, _, width = blocks_ref.shape
    reads = [
        pltpu.make_async_copy(
            rows_ref.at[:, width * chip : width * chip + width], held.at[chip], read_semaphores.at[chip]
        )
        for chip in range(chips)
    ]
    writes = [
        pltpu.make_async_copy(held.at[chip], blocks_ref.at[chip], write_semaphores.at[chip])
        for chip in range(chips)
    ]
    for read in reads:
        read.start()
    for read, write in zip(reads, writes):
        read.wait()
        write.start()
    for write in writes:
        write.wait()


def cut(own_rows, chips):
    rows, cols = own_rows.shape
    width = cols // chips
    if width % 128:
        return own_rows.reshape(rows, chips, width).transpose(1, 0, 2)
    return pl.pallas_call(
        cut_kernel,
        out_shape=jax.ShapeDtypeStruct((chips, rows, width), own_rows.dtype),
        in_specs=[pl.BlockSpec(memory_space=pltpu.HBM)],
        out_specs=pl.BlockSpec(memory_space=pltpu.HBM),
        scratch_shapes=[
            pltpu.VMEM((chips, rows, width), own_rows.dtype),
            pltpu.SemaphoreType.DMA((chips,)),
            pltpu.SemaphoreType.DMA((chips,)),
        ],
        compiler_params=pltpu.CompilerParams(vmem_limit_bytes=66_000_000),
        cost_estimate=pl.CostEstimate(flops=1000, bytes_accessed=4 * rows * cols, transcendentals=0),
        name="cut",
    )(own_rows)


def first_p_kernel(own_ref, other_ref, blocks_ref, p_ref):
    chips, rows, width = blocks_ref.shape
    _, lo, rank, placed = own_ref.shape
    rest = width - placed
    is_even = lax.axis_index("core") == 0
    total = jnp.zeros((rows, rank), jnp.float32)
    for chip in range(chips):
        own, other = own_ref[chip // lo, chip % lo], other_ref[chip // lo, chip % lo]
        even = jnp.where(is_even, own, other)
        odd = jnp.where(is_even, other, own)
        for part, start in ((even, 0), (odd, rest)):
            total += lax.dot_general(
                blocks_ref[chip, :, start : start + placed],
                part,
                (((1,), (1,)), ((), ())),
                preferred_element_type=jnp.float32,
            )
    p_ref[...] = packed_rows(total, 128 // rank)


def next_p_kernel(q_ref, block_ref, p_ref):
    chips, rows, width = block_ref.shape
    rank = q_ref.shape[0]
    groups = 128 // rank
    per = rows // groups
    right = q_ref[...]
    parts = [
        lax.dot_general(
            block_ref[:, per * g : per * g + per, :].reshape(chips * per, width),
            right,
            (((1,), (1,)), ((), ())),
            preferred_element_type=jnp.float32,
        )
        for g in range(groups)
    ]
    p_ref[...] = jnp.concatenate(parts, axis=1).reshape(p_ref.shape)


def gram_kernel(p_ref, gram_ref):
    rank = gram_ref.shape[0]
    packed = p_ref[...]
    wide = lax.dot_general(
        packed, packed, (((0,), (0,)), ((), ())), precision=HIGHEST, preferred_element_type=jnp.float32
    )
    total = wide[:rank, :rank]
    for g in range(1, 128 // rank):
        total += wide[rank * g : rank * g + rank, rank * g : rank * g + rank]
    gram_ref[...] = total


def tiled_inverse_factor(gram, columns):
    rank = gram.shape[0]
    blocks = rank // 8
    for j in range(rank):
        column = jnp.broadcast_to(gram[:, j : j + 1], (rank, 128))
        for i in range(j // 8, blocks):
            columns[j, i] = column[8 * i : 8 * i + 8]
    row = lax.broadcasted_iota(jnp.int32, (8, 128), 0)
    lane = lax.broadcasted_iota(jnp.int32, (8, 128), 1) % rank
    solved = [(lane == row + 8 * i).astype(jnp.float32) for i in range(blocks)]
    for k in range(rank):
        top, at = k // 8, k % 8
        pivot = columns[k, top][at : at + 1]
        scale = lax.rsqrt(pivot)
        scale = scale * (1.5 - 0.5 * pivot * scale * scale)
        lower = {i: columns[k, i] * scale for i in range(top, blocks)}
        lower[top] = jnp.where(row > at, lower[top], 0.0)
        solved_row = solved[top][at : at + 1] * scale
        for i in range(top, blocks):
            reduced = solved[i] - lower[i] * solved_row
            solved[i] = jnp.where(row == at, solved_row, reduced) if i == top else reduced
        for j in range(k + 1, rank):
            entry = lower[j // 8][j % 8 : j % 8 + 1]
            for i in range(j // 8, blocks):
                columns[j, i] = columns[j, i] - lower[i] * entry
    return jnp.concatenate(solved, axis=0)


def basis_kernel(own_gram_ref, other_gram_ref, p_ref, p_own_ref, block_ref, q_ref, basis_ref, columns):
    chips, rows, width = block_ref.shape
    rank = own_gram_ref.shape[0]
    groups = 128 // rank
    per = rows // groups
    inverse = tiled_inverse_factor(own_gram_ref[...] + other_gram_ref[...], columns)
    tall = jnp.concatenate([inverse] * groups, axis=0)
    of_row = lax.broadcasted_iota(jnp.int32, (128, 128), 0) // rank
    of_lane = lax.broadcasted_iota(jnp.int32, (128, 128), 1) // rank
    diagonal = jnp.where(of_row == of_lane, tall, 0.0)
    over_lanes = (((1,), (1,)), ((), ()))
    basis = lax.dot_general(
        p_ref[...], diagonal, over_lanes, precision=HIGHEST, preferred_element_type=jnp.float32
    )
    own = lax.dot_general(
        p_own_ref[...], diagonal, over_lanes, precision=HIGHEST, preferred_element_type=jnp.float32
    )
    for g in range(groups):
        basis_ref[per * g : per * g + per, :] = own[:, rank * g : rank * g + rank]
    left = basis.T.astype(jnp.bfloat16)
    total = jnp.zeros((rank, width), jnp.float32)
    for g in range(groups):
        total += jnp.dot(
            left[rank * g : rank * g + rank],
            block_ref[:, per * g : per * g + per, :].reshape(chips * per, width),
            preferred_element_type=jnp.float32,
        )
    q_ref[...] = total


def gather_chips(values):
    by_hi = spread(values, "hi")
    return spread(by_hi, "lo").swapaxes(0, 1)


def gather_right(q_half):
    blocks = gather_chips(q_half)
    hi, lo, half, width = blocks.shape
    own = blocks.transpose(2, 0, 1, 3).reshape(half, hi * lo * width)
    return own, swap_cores(own)


def on_device(accumulated, q_start):
    own_rows = accumulated[0]
    replicas = lax.axis_size("rep")
    chips = lax.axis_size(CHIP)
    core = lax.axis_index("core")
    rows, cols = own_rows.shape
    rank, shard_cols = q_start.shape
    half, width, per = rank // 2, cols // chips, rows * rank // 128
    f32, bf16 = jnp.float32, jnp.bfloat16

    blocks = cut(own_rows, chips)
    block = lax.all_to_all(blocks, CHIP, 0, 0, tiled=True)

    shift = shard_cols % 128
    placed = jnp.where(
        core == 0, jnp.pad(q_start, ((0, 0), (0, shift))), jnp.pad(q_start, ((0, 0), (shift, 0)))
    )
    by_hi = exchanged(placed, "hi", 0)
    own = exchanged(by_hi, "lo", 1)
    other = swap_cores(own)
    p_own = kernel_call(
        first_p_kernel, jax.ShapeDtypeStruct((per, 128), f32), 2 * rows * rank * cols
    )(own, other, blocks)
    for iteration in range(ITERS):
        if iteration > 0:
            term = kernel_call(
                next_p_kernel, jax.ShapeDtypeStruct((chips, per, 128), f32), 2 * chips * rows * rank * width
            )(right_factor, block)
            p_own = jnp.sum(lax.all_to_all(term, CHIP, 0, 0, tiled=True), axis=0)
        if replicas > 1:
            p_own = lax.psum(p_own, "rep")
        if iteration > 0:
            p_chip = spread(p_own, CHIP)
        else:
            by_lo = exchanged(p_own, "lo", 0)
            p_chip = exchanged(by_lo, "hi", 0)
        p_rows = p_chip.reshape(chips * per, 128)
        own_gram = kernel_call(
            gram_kernel, jax.ShapeDtypeStruct((rank, rank), f32), 2 * chips * per * 128 * 128
        )(p_rows)
        q_term, basis = kernel_call(
            basis_kernel,
            (jax.ShapeDtypeStruct((rank, width), f32), jax.ShapeDtypeStruct((rows, rank), f32)),
            2 * chips * rows * rank * width,
            [pltpu.VMEM((rank, rank // 8, 8, 128), f32)],
        )(own_gram, swap_cores(own_gram), p_rows, p_own, block)
        q_chip = q_term + swap_cores(q_term)
        if replicas > 1:
            q_chip = lax.psum(q_chip, "rep")
        q_chip = q_chip / replicas
        right_factor = q_chip.astype(bf16)
    q_owned = lax.dynamic_slice_in_dim(q_chip, core * shard_cols, shard_cols, 1)
    own, other = gather_right(lax.dynamic_slice_in_dim(right_factor, core * half, half, 0))
    basis_bf16 = basis.astype(bf16)
    mine = lax.dynamic_slice_in_dim(basis_bf16, core * half, half, 1)
    theirs = lax.dynamic_slice_in_dim(basis_bf16, (1 - core) * half, half, 1)
    approx = lax.dot_general(
        jnp.concatenate([mine, theirs], axis=1),
        jnp.concatenate([own, other], axis=0),
        (((1,), (0,)), ((), ())),
        preferred_element_type=f32,
    )
    residual_buffer = (own_rows.astype(f32) - approx).astype(bf16)[None]
    return (residual_buffer, basis, q_owned)


def solution(mesh):
    chips = mesh.shape["fsdp"] // 2
    lo = 4
    split = Mesh(
        mesh.devices.reshape(mesh.shape["rep"], chips // lo, lo, 2), ("rep", "hi", "lo", "core")
    )
    in_specs = (P("rep", ROWS, None), P(None, ROWS))
    out_specs = (P("rep", ROWS, None), P(ROWS, None), P(None, ROWS))
    return jax.shard_map(
        on_device, mesh=split, in_specs=in_specs, out_specs=out_specs, check_vma=False
    )
```

```python
import jax
import jax.numpy as jnp
from jax import lax
from jax.experimental import pallas as pl
from jax.experimental.pallas import tpu as pltpu
from jax.sharding import Mesh, PartitionSpec as P


ITERS = 2
HIGHEST = lax.Precision.HIGHEST
CHIP = ("hi", "lo")
ROWS = ("hi", "lo", "core")
SWAP = ((0, 1), (1, 0))


def swap_cores(values):
    return lax.ppermute(values, "core", SWAP)


def spread(values, axis):
    copies = jnp.broadcast_to(values[None], (lax.axis_size(axis),) + values.shape)
    return lax.all_to_all(copies, axis, 0, 0, tiled=True)


def exchanged(values, axis, dim):
    position = lax.axis_index(axis)
    size = lax.axis_size(axis)
    pieces = [values]
    for offset in range(1, size):
        pairs = tuple((index, index ^ offset) for index in range(size))
        pieces.append(lax.ppermute(values, axis, pairs))
    bit = 1
    while bit < size:
        swap = (position & bit) != 0
        pieces = [jnp.where(swap, pieces[i ^ bit], pieces[i]) for i in range(size)]
        bit *= 2
    return jnp.stack(pieces, axis=dim)


def kernel_call(kernel, out_shape, flops, scratch=()):
    single = not isinstance(out_shape, tuple)
    outs = (out_shape,) if single else out_shape
    vmem = pl.BlockSpec(memory_space=pltpu.VMEM)
    return lambda *args: pl.pallas_call(
        kernel,
        out_shape=out_shape,
        in_specs=[vmem] * len(args),
        out_specs=vmem if single else (vmem,) * len(outs),
        scratch_shapes=list(scratch),
        compiler_params=pltpu.CompilerParams(vmem_limit_bytes=16 * 1024 * 1024),
        cost_estimate=pl.CostEstimate(
            flops=flops, bytes_accessed=sum(a.size * a.dtype.itemsize for a in args), transcendentals=0
        ),
    )(*args)


def packed_rows(wide, groups):
    per = wide.shape[0] // groups
    return jnp.concatenate([wide[per * g : per * g + per, :] for g in range(groups)], axis=1)


def cut_kernel(rows_ref, blocks_ref, held, read_semaphores, write_semaphores):
    chips, _, width = blocks_ref.shape
    reads = [
        pltpu.make_async_copy(
            rows_ref.at[:, width * chip : width * chip + width], held.at[chip], read_semaphores.at[chip]
        )
        for chip in range(chips)
    ]
    writes = [
        pltpu.make_async_copy(held.at[chip], blocks_ref.at[chip], write_semaphores.at[chip])
        for chip in range(chips)
    ]
    for read in reads:
        read.start()
    for read, write in zip(reads, writes):
        read.wait()
        write.start()
    for write in writes:
        write.wait()


def cut(own_rows, chips):
    rows, cols = own_rows.shape
    width = cols // chips
    if width % 128:
        return own_rows.reshape(rows, chips, width).transpose(1, 0, 2)
    return pl.pallas_call(
        cut_kernel,
        out_shape=jax.ShapeDtypeStruct((chips, rows, width), own_rows.dtype),
        in_specs=[pl.BlockSpec(memory_space=pltpu.HBM)],
        out_specs=pl.BlockSpec(memory_space=pltpu.HBM),
        scratch_shapes=[
            pltpu.VMEM((chips, rows, width), own_rows.dtype),
            pltpu.SemaphoreType.DMA((chips,)),
            pltpu.SemaphoreType.DMA((chips,)),
        ],
        compiler_params=pltpu.CompilerParams(vmem_limit_bytes=66_000_000),
        cost_estimate=pl.CostEstimate(flops=1000, bytes_accessed=4 * rows * cols, transcendentals=0),
        name="cut",
    )(own_rows)


def first_p_kernel(own_ref, other_ref, rows_ref, p_ref):
    rows, cols = rows_ref.shape
    hi, lo, rank, placed = own_ref.shape
    chips = hi * lo
    width = cols // chips
    rest = width - placed
    is_even = lax.axis_index("core") == 0
    total = jnp.zeros((rows, rank), jnp.float32)
    for chip in range(chips):
        own, other = own_ref[chip // lo, chip % lo], other_ref[chip // lo, chip % lo]
        even = jnp.where(is_even, own, other)
        odd = jnp.where(is_even, other, own)
        for part, start in ((even, 0), (odd, rest)):
            total += lax.dot_general(
                rows_ref[:, width * chip + start : width * chip + start + placed],
                part,
                (((1,), (1,)), ((), ())),
                preferred_element_type=jnp.float32,
            )
    p_ref[...] = packed_rows(total, 128 // rank)


def next_p_kernel(q_ref, block_ref, p_ref):
    chips, rows, width = block_ref.shape
    rank = q_ref.shape[0]
    groups = 128 // rank
    per = rows // groups
    right = q_ref[...]
    parts = [
        lax.dot_general(
            block_ref[:, per * g : per * g + per, :].reshape(chips * per, width),
            right,
            (((1,), (1,)), ((), ())),
            preferred_element_type=jnp.float32,
        )
        for g in range(groups)
    ]
    p_ref[...] = jnp.concatenate(parts, axis=1).reshape(p_ref.shape)


def gram_kernel(p_ref, gram_ref):
    rank = gram_ref.shape[0]
    packed = p_ref[...]
    wide = lax.dot_general(
        packed, packed, (((0,), (0,)), ((), ())), precision=HIGHEST, preferred_element_type=jnp.float32
    )
    total = wide[:rank, :rank]
    for g in range(1, 128 // rank):
        total += wide[rank * g : rank * g + rank, rank * g : rank * g + rank]
    gram_ref[...] = total


def tiled_inverse_factor(gram, columns):
    rank = gram.shape[0]
    blocks = rank // 8
    for j in range(rank):
        column = jnp.broadcast_to(gram[:, j : j + 1], (rank, 128))
        for i in range(j // 8, blocks):
            columns[j, i] = column[8 * i : 8 * i + 8]
    row = lax.broadcasted_iota(jnp.int32, (8, 128), 0)
    lane = lax.broadcasted_iota(jnp.int32, (8, 128), 1) % rank
    solved = [(lane == row + 8 * i).astype(jnp.float32) for i in range(blocks)]
    for k in range(rank):
        top, at = k // 8, k % 8
        pivot = columns[k, top][at : at + 1]
        scale = lax.rsqrt(pivot)
        scale = scale * (1.5 - 0.5 * pivot * scale * scale)
        lower = {i: columns[k, i] * scale for i in range(top, blocks)}
        lower[top] = jnp.where(row > at, lower[top], 0.0)
        solved_row = solved[top][at : at + 1] * scale
        for i in range(top, blocks):
            reduced = solved[i] - lower[i] * solved_row
            solved[i] = jnp.where(row == at, solved_row, reduced) if i == top else reduced
        for j in range(k + 1, rank):
            entry = lower[j // 8][j % 8 : j % 8 + 1]
            for i in range(j // 8, blocks):
                columns[j, i] = columns[j, i] - lower[i] * entry
    return jnp.concatenate(solved, axis=0)


def diagonal_of(inverse, groups):
    rank = inverse.shape[0]
    tall = jnp.concatenate([inverse] * groups, axis=0)
    of_row = lax.broadcasted_iota(jnp.int32, (128, 128), 0) // rank
    of_lane = lax.broadcasted_iota(jnp.int32, (128, 128), 1) // rank
    return jnp.where(of_row == of_lane, tall, 0.0)


def basis_kernel(own_gram_ref, other_gram_ref, p_ref, block_ref, q_ref, inverse_ref, columns):
    chips, rows, width = block_ref.shape
    rank = own_gram_ref.shape[0]
    groups = 128 // rank
    per = rows // groups
    inverse = tiled_inverse_factor(own_gram_ref[...] + other_gram_ref[...], columns)
    inverse_ref[...] = inverse
    basis = lax.dot_general(
        p_ref[...],
        diagonal_of(inverse, groups),
        (((1,), (1,)), ((), ())),
        precision=HIGHEST,
        preferred_element_type=jnp.float32,
    )
    left = basis.T.astype(jnp.bfloat16)
    total = jnp.zeros((rank, width), jnp.float32)
    for g in range(groups):
        total += jnp.dot(
            left[rank * g : rank * g + rank],
            block_ref[:, per * g : per * g + per, :].reshape(chips * per, width),
            preferred_element_type=jnp.float32,
        )
    q_ref[...] = total


def own_basis_kernel(inverse_ref, p_own_ref, basis_ref, rounded_ref):
    rank = inverse_ref.shape[0]
    groups = 128 // rank
    own = lax.dot_general(
        p_own_ref[...],
        diagonal_of(inverse_ref[...], groups),
        (((1,), (1,)), ((), ())),
        precision=HIGHEST,
        preferred_element_type=jnp.float32,
    ).T
    own = jnp.concatenate([own[rank * g : rank * g + rank] for g in range(groups)], axis=1)
    basis_ref[...] = own
    rounded_ref[...] = own.astype(rounded_ref.dtype)


def fetch_kernel(rows_ref, held_ref, semaphores):
    parts = semaphores.shape[0]
    span = rows_ref.shape[0] // parts
    copies = [
        pltpu.make_async_copy(
            rows_ref.at[span * i : span * i + span], held_ref.at[span * i : span * i + span], semaphores.at[i]
        )
        for i in range(parts)
    ]
    for copy in copies:
        copy.start()
    for copy in copies:
        copy.wait()


def fetch(own_rows):
    parts = 4
    return pl.pallas_call(
        fetch_kernel,
        out_shape=jax.ShapeDtypeStruct(own_rows.shape, own_rows.dtype),
        in_specs=[pl.BlockSpec(memory_space=pltpu.HBM)],
        out_specs=pl.BlockSpec(memory_space=pltpu.VMEM),
        scratch_shapes=[pltpu.SemaphoreType.DMA((parts,))],
        compiler_params=pltpu.CompilerParams(vmem_limit_bytes=54_000_000),
        cost_estimate=pl.CostEstimate(
            flops=1000000, bytes_accessed=2 * own_rows.size * own_rows.dtype.itemsize, transcendentals=0
        ),
        name="fetch",
    )(own_rows)


def residual_kernel(own_ref, other_ref, left_ref, q_ref, rows_ref, residual_ref, q_owned_ref, given, writes):
    chips, _, width = own_ref.shape
    parts, _, span = given.shape
    shard_cols = q_owned_ref.shape[1]
    copies = [
        pltpu.make_async_copy(given.at[i], residual_ref.at[:, span * i : span * i + span], writes.at[i])
        for i in range(parts)
    ]
    is_first = lax.axis_index("core") == 0
    left = left_ref[...]
    for i in range(parts):
        for place in range(chips // parts):
            chip = i * (chips // parts) + place
            own, other = own_ref[chip], other_ref[chip]
            right = jnp.concatenate(
                [jnp.where(is_first, own, other), jnp.where(is_first, other, own)], axis=0
            )
            approx = lax.dot_general(
                left, right, (((0,), (0,)), ((), ())), preferred_element_type=jnp.float32
            )
            kept = rows_ref[:, width * chip : width * chip + width].astype(jnp.float32)
            given[i, :, width * place : width * place + width] = (kept - approx).astype(given.dtype)
        copies[i].start()
    q_owned_ref[...] = jnp.where(is_first, q_ref[:, :shard_cols], q_ref[:, shard_cols:])
    for copy in copies:
        copy.wait()


def residual_and_columns(own, other, left, q_chip, own_rows, shard_cols):
    rows, cols = own_rows.shape
    parts = 8
    vmem, hbm = pl.BlockSpec(memory_space=pltpu.VMEM), pl.BlockSpec(memory_space=pltpu.HBM)
    return pl.pallas_call(
        residual_kernel,
        out_shape=(
            jax.ShapeDtypeStruct((rows, cols), own_rows.dtype),
            jax.ShapeDtypeStruct((q_chip.shape[0], shard_cols), jnp.float32),
        ),
        in_specs=[vmem] * 5,
        out_specs=(hbm, vmem),
        scratch_shapes=[
            pltpu.VMEM((parts, rows, cols // parts), own_rows.dtype),
            pltpu.SemaphoreType.DMA((parts,)),
        ],
        compiler_params=pltpu.CompilerParams(vmem_limit_bytes=16 * 1024 * 1024),
        cost_estimate=pl.CostEstimate(
            flops=2 * rows * cols * q_chip.shape[0], bytes_accessed=4 * rows * cols, transcendentals=0
        ),
        name="residual",
    )(own, other, left, q_chip, own_rows)


def on_device(accumulated, q_start):
    own_rows = accumulated[0]
    replicas = lax.axis_size("rep")
    chips = lax.axis_size(CHIP)
    core = lax.axis_index("core")
    rows, cols = own_rows.shape
    rank, shard_cols = q_start.shape
    half, width, per = rank // 2, cols // chips, rows * rank // 128
    f32, bf16 = jnp.float32, jnp.bfloat16

    blocks = cut(own_rows, chips)
    block = lax.all_to_all(blocks, CHIP, 0, 0, tiled=True)

    shift = shard_cols % 128
    placed = jnp.where(
        core == 0, jnp.pad(q_start, ((0, 0), (0, shift))), jnp.pad(q_start, ((0, 0), (shift, 0)))
    )
    by_hi = exchanged(placed, "hi", 0)
    own = exchanged(by_hi, "lo", 1)
    other = swap_cores(own)
    p_own = kernel_call(
        first_p_kernel, jax.ShapeDtypeStruct((per, 128), f32), 2 * rows * rank * cols
    )(own, other, own_rows)
    for iteration in range(ITERS):
        if iteration > 0:
            term = kernel_call(
                next_p_kernel, jax.ShapeDtypeStruct((chips, per, 128), f32), 2 * chips * rows * rank * width
            )(right_factor, block)
            p_own = jnp.sum(lax.all_to_all(term, CHIP, 0, 0, tiled=True), axis=0)
        if replicas > 1:
            p_own = lax.psum(p_own, "rep")
        if iteration > 0:
            p_chip = spread(p_own, CHIP)
        else:
            by_lo = exchanged(p_own, "lo", 0)
            p_chip = exchanged(by_lo, "hi", 0)
        p_rows = p_chip.reshape(chips * per, 128)
        own_gram = kernel_call(
            gram_kernel, jax.ShapeDtypeStruct((rank, rank), f32), 2 * chips * per * 128 * 128
        )(p_rows)
        q_term, inverse = kernel_call(
            basis_kernel,
            (jax.ShapeDtypeStruct((rank, width), f32), jax.ShapeDtypeStruct((rank, 128), f32)),
            2 * chips * rows * rank * width,
            [pltpu.VMEM((rank, rank // 8, 8, 128), f32)],
        )(own_gram, swap_cores(own_gram), p_rows, block)
        q_chip = q_term + swap_cores(q_term)
        if replicas > 1:
            q_chip = lax.psum(q_chip, "rep")
        q_chip = q_chip / replicas
        right_factor = q_chip.astype(bf16)
    basis, rounded = kernel_call(
        own_basis_kernel,
        (jax.ShapeDtypeStruct((rank, rows), f32), jax.ShapeDtypeStruct((rank, rows), bf16)),
        2 * per * 128 * 128,
    )(inverse, p_own)
    own = spread(lax.dynamic_slice_in_dim(right_factor, core * half, half, 0)[None], CHIP)
    own = own.reshape(chips, half, width)
    own, later_rows = lax.optimization_barrier((own, own_rows))
    residual, q_owned = residual_and_columns(
        own, swap_cores(own), rounded, q_chip, fetch(later_rows), shard_cols
    )
    return (residual[None], basis.T, q_owned)


def solution(mesh):
    chips = mesh.shape["fsdp"] // 2
    lo = 4
    split = Mesh(
        mesh.devices.reshape(mesh.shape["rep"], chips // lo, lo, 2), ("rep", "hi", "lo", "core")
    )
    in_specs = (P("rep", ROWS, None), P(None, ROWS))
    out_specs = (P("rep", ROWS, None), P(ROWS, None), P(None, ROWS))
    return jax.shard_map(
        on_device, mesh=split, in_specs=in_specs, out_specs=out_specs, check_vma=False
    )
```
